32 devices in a mesh: row: 4 (over y, core), col: 8 (over z, x).
Axes of the slice: x: 2, y: 2, z: 4, core: 2. Of those that a mesh axis runs over, the one named last changes fastest.
Arguments:
- adjacency: int32 [3392, 3392], P('row', 'col'), may hold values from 0 to 3
- degree: int32 [3392], replicated, may hold values from 64 to 511
- cotangent: bfloat16 [3392, 512], P(('row', 'col')), may hold values from -6 to 6
- features: bfloat16 [3392, 512], P('col'), may hold values from -0.029907227 to 0.029907227
- weight: bfloat16 [512, 512], replicated, may hold values from -0.25 to 0.25
Outputs:
- grad_input: bfloat16 [3392, 512], P('col', 'row')
- grad_weight: float32 [512, 512], P('col', 'row')
The draws below stay inside these ranges and needn't reach their ends.
All inputs are finite; a program needn't handle non-finite values.
Results may differ from the reference program's by a relative error of at most 0.0058.
Values may be sent and summed in bfloat16 or wider, within the bound.
A program may use at most 128 MiB of HBM per device.

```python
import jax
import jax.numpy as jnp
from jax import lax

F = 512
NODES = 3392
N_ROW = 4


def with_ends(array, own_key, least, high):
    longest = array.shape.index(max(array.shape))
    spots = []
    for shift in (0, 1):
        where = [jax.random.randint(jax.random.fold_in(own_key, axis), (), 0, length) for axis, length in enumerate(array.shape)]
        where[longest] = (where[longest] + shift) % array.shape[longest]
        spots.append(tuple(where))
    return array.at[spots[0]].set(least).at[spots[1]].set(high)


def spiked(array, own_key, source, target, parts, factor):
    owner, partner = [(jnp.arange(array.shape[dim]) // (array.shape[dim] // parts)).reshape([-1 if axis == dim else 1 for axis in range(array.ndim)]) for dim in (source, target)]
    chosen = jax.random.permutation(own_key, parts)[partner]
    strong = (owner == chosen) | (owner == (partner + parts // 2) % parts)
    return jnp.where(strong, factor * array, array)


def block_levels(rng, shape, shards, low, largest):
    def one(position, blocks):
        draws = jax.random.uniform(jax.random.fold_in(jax.random.fold_in(rng, 6), position), (blocks,), jnp.float32, low / len(shards), largest / len(shards))
        return jnp.repeat(jnp.exp(draws), shape[position] // blocks).reshape((-1,) + (1,) * (len(shape) - position - 1))

    gain = one(*shards[0])
    for cut in shards[1:]:
        gain = gain * one(*cut)
    return gain


def noise(key, shape, spread, reach, cuts=(), kind=jnp.bfloat16):
    entries = jax.random.normal(key, shape, jnp.float32) * spread
    if len(cuts) > 0:
        entries = block_levels(key, shape, cuts, -0.22, 0.18) * entries
    return jnp.clip(entries, min=-reach, max=reach).astype(kind)


def bell_draw_with(rng, shape, deviation, most, cuts, heavy, kind=jnp.bfloat16):
    drawn = deviation * jax.random.normal(rng, shape, jnp.float32)
    if cuts:
        drawn = drawn * block_levels(rng, shape, cuts, -0.22, 0.18)
    return jnp.clip(spiked(drawn, jax.random.fold_in(rng, 3), *heavy), -most, most).astype(kind)


def setup_inputs(seed: int = 0) -> dict:
    streams_of = jax.random.split(jax.random.key(seed), 6)
    adjacency = with_ends(jax.random.randint(streams_of[0], (NODES, NODES), 0, 4), jax.random.fold_in(streams_of[0], 1), 0, 3).astype(jnp.int32)
    degree = with_ends(jax.random.randint(streams_of[1], (NODES,), 64, 512), jax.random.fold_in(streams_of[1], 1), 64, 511).astype(jnp.int32)
    cotangent = noise(streams_of[2], (NODES, F), 1.0, 6.0, ((0, 32),))
    features = bell_draw_with(streams_of[3], (NODES, F), 0.005, 0.029907227, ((0, 8),), (0, 1, 8, 2.0))
    weight = noise(streams_of[4], (F, F), F ** -0.5, 0.25)
    return dict(adjacency=adjacency, degree=degree, cotangent=cotangent, features=features, weight=weight)


def reference(adjacency, degree, cotangent, features, weight):
    inv_root = lax.rsqrt(degree.astype(jnp.float32))
    scaled = (cotangent.astype(jnp.float32) * inv_root[:, None]).astype(jnp.bfloat16)
    scaled = lax.optimization_barrier(scaled).astype(jnp.float32)
    step_rows = NODES // N_ROW

    def accumulate(total, index):
        start = (index * step_rows).astype(jnp.int32)
        tile = lax.dynamic_slice_in_dim(adjacency, start, step_rows, 0).astype(jnp.float32)
        block = lax.dynamic_slice_in_dim(scaled, start, step_rows, 0)
        term = jnp.dot(tile.T, block, precision=lax.Precision.HIGHEST, preferred_element_type=jnp.float32)
        return (total + term, None)
    total, _ = lax.scan(accumulate, jnp.zeros((NODES, F), jnp.float32), jnp.arange(N_ROW, dtype=jnp.int32))
    grad_z = (total * inv_root[:, None]).astype(jnp.bfloat16)
    grad_input = jnp.dot(grad_z, weight.T, preferred_element_type=jnp.float32).astype(jnp.bfloat16)
    grad_weight = jnp.dot(features.T, grad_z, preferred_element_type=jnp.float32)
    return (grad_input, grad_weight)
```

```python
import functools

import jax
import jax.numpy as jnp
from jax import lax
from jax.experimental import pallas as pl
from jax.experimental.pallas import tpu as pltpu
from jax.sharding import PartitionSpec as P

MESH = pl.DeviceIdType.MESH
F32, BF16 = jnp.float32, jnp.bfloat16
CORES = 2


def up(size, unit):
    return -(-size // unit) * unit


def inner_of(count):
    return max(d for d in range(1, count + 1) if count % d == 0 and d * d <= count)


def kernel(
    R, C, block,
    x_ref, a_hbm, f_hbm, w_hbm, scale_ref, gi_ref, gw_ref,
    a_v, f_v, w_v, at, ft, s_v, mine, part, theirs, z_all, wt, wrec,
    load_sem, swap_sem, own_sem, pair_sem, got_sem, fwd_sem,
    part_send, part_recv, z_send, z_recv, z_fwd, wt_send, wt_recv,
):
    I = inner_of(C)
    O = C // I
    Y = R // CORES
    rows, n = a_v.shape
    padded, share = x_ref.shape[1:]
    slot = s_v.shape[3]
    r = lax.axis_index("row")
    c = lax.axis_index("col")
    y, k = r // CORES, r % CORES
    o, i = c // I, c % I
    mate = y * CORES + (1 - k)
    outer = [lax.rem(o + d, O) * I + i for d in range(1, O)]
    inner = [o * I + lax.rem(i + d, I) for d in range(1, I)]
    others = [lax.rem(c + d, C) for d in range(1, C)]
    y_at = [lax.rem(y + 1 + s, Y) for s in range(Y)]

    def remote(src, dst, send, recv, row, col):
        return pltpu.make_async_remote_copy(
            src_ref=src, dst_ref=dst, send_sem=send, recv_sem=recv,
            device_id=(row, col), device_id_type=MESH,
        )

    def await_bytes(ref, sem):
        pltpu.make_async_copy(ref, ref, sem).wait()

    load_a = pltpu.make_async_copy(a_hbm, a_v, load_sem.at[0])
    load_f = pltpu.make_async_copy(f_hbm, f_v, load_sem.at[1])
    load_w = pltpu.make_async_copy(
        w_hbm.at[pl.ds(pl.multiple_of(r * share, share), share), :], w_v, load_sem.at[2]
    )
    load_a.start()
    load_f.start()
    load_w.start()

    barrier = pltpu.get_barrier_semaphore()
    peers = [(r, p) for p in others] + [(mate, p) for p in outer + inner] + [(mate, c)]
    peers += [(yy * CORES + k, c) for yy in y_at[:-1]]
    for row, col in peers:
        pl.semaphore_signal(barrier, inc=1, device_id=(row, col), device_id_type=MESH)
    pl.semaphore_wait(barrier, len(peers))

    live = pl.ds(0, padded)
    for s in range(Y):
        same = x_ref.at[y_at[s] * CORES + k]
        cross = x_ref.at[y_at[s] * CORES + (1 - k)]
        for p in outer + inner:
            remote(same, s_v.at[s, 0, c, live], own_sem.at[s, 0], got_sem.at[s, c], r, p).start()
            remote(cross, s_v.at[s, 1, c, live], own_sem.at[s, 1], got_sem.at[s, c], mate, p).start()
        remote(cross, s_v.at[s, 1, c, live], pair_sem.at[s], got_sem.at[s, c], mate, c).start()
        s_v[s, 0, c, 0:padded, :] = x_ref[y_at[s] * CORES + k]
    if slot > padded:
        for s in range(Y):
            s_v[s, :, :, padded:slot, :] = jnp.zeros((CORES, C, slot - padded, share), BF16)

    load_a.wait()
    for j in range(C):
        tile = a_v[j * block:(j + 1) * block, :].astype(F32)
        if slot > block:
            tile = jnp.concatenate([tile, jnp.zeros((slot - block, n), F32)], axis=0)
        at[0, :, j * slot:(j + 1) * slot] = tile.T.astype(BF16)
    swap = remote(at.at[0], at.at[1], swap_sem.at[0], swap_sem.at[1], mate, c)
    swap.start()
    load_f.wait()
    ft[...] = f_v[...].astype(F32).T.astype(BF16)

    group = min(C, 8)

    def forward(s):
        for d, p in enumerate(outer):
            await_bytes(s_v.at[s, :, p, live], got_sem.at[s, p])
            for q in inner:
                remote(
                    s_v.at[s, :, p, live], s_v.at[s, :, p, live],
                    fwd_sem.at[s, d], got_sem.at[s, p], r, q,
                ).start()

    def gathered(s):
        await_bytes(s_v.at[s, 1, c, live], got_sem.at[s, c])
        for e in range(1, I):
            for d in range(O):
                p = lax.rem(o + d, O) * I + lax.rem(i + e, I)
                await_bytes(s_v.at[s, :, p, live], got_sem.at[s, p])

    def product(s):
        def term(t, g):
            left = at[t, :, pl.ds(pl.multiple_of(g * group * slot, group * slot), group * slot)]
            right = s_v[s, t, pl.ds(g * group, group)].reshape(group * slot, share)
            return jnp.dot(left, right, preferred_element_type=F32)

        if C == group:
            mine[...] = term(0, 0) + term(1, 0)
        else:
            mine[...] = jnp.zeros_like(mine)

            @pl.loop(0, C // group)
            def _(g):
                mine[...] += term(0, g) + term(1, g)

    for s in range(Y):
        forward(s)
        gathered(s)
        if s == 0:
            swap.wait()
        product(s)
        if s < Y - 1:
            part[s] = mine[...]
            remote(
                part.at[s], theirs.at[s], part_send.at[s], part_recv.at[s], y_at[s] * CORES + k, c
            ).start()

    total = mine[...]
    for s in range(Y - 1):
        await_bytes(theirs.at[s], part_recv.at[s])
        total = total + theirs[s]
    z_mine = (total * scale_ref[...]).astype(BF16)
    z_all[r] = z_mine
    z_here = z_all.at[r]
    for s in range(Y - 1):
        remote(z_here, z_here, z_send.at[s], z_recv.at[r], y_at[s] * CORES + k, c).start()
    remote(z_here, z_here, z_send.at[Y - 1], z_recv.at[r], mate, c).start()

    term = jnp.dot(ft[...], z_mine, preferred_element_type=F32)
    wt[...] = term.reshape(wt.shape)
    for p in others:
        remote(wt.at[p], wrec.at[c], wt_send.at[0], wt_recv.at[c], r, p).start()

    for s in range(Y - 1):
        q = y_at[s] * CORES + k
        await_bytes(z_all.at[q], z_recv.at[q])
        remote(z_all.at[q], z_all.at[q], z_fwd.at[s], z_recv.at[q], mate, c).start()
    load_w.wait()
    for s in range(Y):
        q = y_at[s] * CORES + (1 - k)
        await_bytes(z_all.at[q], z_recv.at[q])
    out = jnp.zeros((n, share), F32)
    for q in range(R):
        out = out + lax.dot_general(
            z_all[q], w_v[:, q * share:(q + 1) * share],
            (((1,), (1,)), ((), ())), preferred_element_type=F32,
        )
    gi_ref[...] = out.astype(BF16)

    gw = wt[c]
    for p in others:
        await_bytes(wrec.at[p], wt_recv.at[p])
        gw = gw + wrec[p]
    gw_ref[...] = gw

    for s in range(Y):
        for t in range(CORES):
            await_bytes(s_v.at[s, t, pl.ds(0, O - 1 + I - 1), live], own_sem.at[s, t])
        await_bytes(s_v.at[s, 1, 0, live], pair_sem.at[s])
        if I > 1:
            for d in range(O - 1):
                await_bytes(s_v.at[s, :, pl.ds(0, I - 1), live], fwd_sem.at[s, d])
    for s in range(Y - 1):
        await_bytes(part.at[s], part_send.at[s])
        await_bytes(z_here, z_fwd.at[s])
    for s in range(Y):
        await_bytes(z_here, z_send.at[s])
    await_bytes(wt.at[pl.ds(0, C - 1)], wt_send.at[0])


def per_device(R, C, adjacency, degree, cotangent, features, weight):
    rows, n = adjacency.shape
    block, width = cotangent.shape
    share = width // R
    padded, slot = up(block, 16), up(block, 128)
    I = inner_of(C)
    O, Y = C // I, R // CORES
    row_index, col_index = lax.axis_index("row"), lax.axis_index("col")
    inv_root = lax.rsqrt(degree.astype(F32))
    row_scale = lax.dynamic_slice_in_dim(inv_root, row_index * rows + col_index * block, block, 0)
    col_scale = lax.dynamic_slice_in_dim(inv_root, col_index * n, n, 0)
    scaled = (cotangent.astype(F32) * row_scale[:, None]).astype(BF16)
    scaled = jnp.pad(scaled, ((0, padded - block), (0, 0)))
    pieces = scaled.reshape(padded, R, share).transpose(1, 0, 2)
    vmem = pl.BlockSpec(memory_space=pltpu.VMEM)
    hbm = pl.BlockSpec(memory_space=pl.ANY)
    dma = pltpu.SemaphoreType.DMA
    return pl.pallas_call(
        functools.partial(kernel, R, C, block),
        out_shape=(
            jax.ShapeDtypeStruct((n, width // R), BF16),
            jax.ShapeDtypeStruct((width // C, share), F32),
        ),
        in_specs=[vmem, hbm, hbm, hbm, vmem],
        out_specs=(vmem, vmem),
        scratch_shapes=[
            pltpu.VMEM((rows, n), jnp.int32),
            pltpu.VMEM((n, width), BF16),
            pltpu.VMEM((share, width), BF16),
            pltpu.VMEM((CORES, n, C * slot), BF16),
            pltpu.VMEM((width, n), BF16),
            pltpu.VMEM((Y, CORES, C, slot, share), BF16),
            pltpu.VMEM((n, share), F32),
            pltpu.VMEM((max(Y - 1, 1), n, share), F32),
            pltpu.VMEM((max(Y - 1, 1), n, share), F32),
            pltpu.VMEM((R, n, share), BF16),
            pltpu.VMEM((C, width // C, share), F32),
            pltpu.VMEM((C, width // C, share), F32),
            dma((3,)),
            dma((2,)),
            dma((Y, CORES)),
            dma((Y,)),
            dma((Y, C)),
            dma((Y, max(O - 1, 1))),
            dma((max(Y - 1, 1),)),
            dma((max(Y - 1, 1),)),
            dma((Y,)),
            dma((R,)),
            dma((max(Y - 1, 1),)),
            dma((1,)),
            dma((C,)),
        ],
        compiler_params=pltpu.CompilerParams(
            collective_id=0, has_side_effects=True, vmem_limit_bytes=60 * 1024 * 1024
        ),
    )(pieces, adjacency, features, weight, col_scale[:, None])


def solution(mesh):
    placed = (P("row", "col"), P(), P(("row", "col"), None), P("col", None), P())
    return jax.shard_map(
        functools.partial(per_device, mesh.shape["row"], mesh.shape["col"]),
        mesh=mesh,
        in_specs=placed,
        out_specs=(P("col", "row"), P("col", "row")),
        check_vma=False,
    )
```

```python
import functools

import jax
import jax.numpy as jnp
from jax import lax
from jax.experimental import pallas as pl
from jax.experimental.pallas import tpu as pltpu
from jax.sharding import PartitionSpec as P

MESH = pl.DeviceIdType.MESH
F32, BF16 = jnp.float32, jnp.bfloat16
CORES = 2


def up(size, unit):
    return -(-size // unit) * unit


def inner_of(count):
    return max(d for d in range(1, count + 1) if count % d == 0 and d * d <= count)


def kernel(
    R, C, block,
    cot_ref, degree_ref, a_hbm, f_hbm, w_hbm, gi_ref, gw_ref,
    d_v, x_ref, a_v, f_v, w_v, at, ft, s_v, mine, part, theirs, z_all, wt, wrec,
    load_sem, swap_sem, own_sem, pair_sem, got_sem, fwd_sem,
    part_send, part_recv, z_send, z_recv, z_fwd, wt_send, wt_recv,
):
    I = inner_of(C)
    O = C // I
    Y = R // CORES
    n, rows = a_v.shape
    padded, share = x_ref.shape[1:]
    slot = s_v.shape[3]
    r = lax.axis_index("row")
    c = lax.axis_index("col")
    y, k = r // CORES, r % CORES
    o, i = c // I, c % I
    mate = y * CORES + (1 - k)
    outer = [lax.rem(o + d, O) * I + i for d in range(1, O)]
    inner = [o * I + lax.rem(i + d, I) for d in range(1, I)]
    others = [lax.rem(c + d, C) for d in range(1, C)]
    y_at = [lax.rem(y + 1 + s, Y) for s in range(Y)]

    def remote(src, dst, send, recv, row, col):
        return pltpu.make_async_remote_copy(
            src_ref=src, dst_ref=dst, send_sem=send, recv_sem=recv,
            device_id=(row, col), device_id_type=MESH,
        )

    def await_bytes(ref, sem):
        pltpu.make_async_copy(ref, ref, sem).wait()

    load_a = pltpu.make_async_copy(a_hbm, a_v, load_sem.at[0])
    load_f = pltpu.make_async_copy(f_hbm, f_v, load_sem.at[1])
    load_w = pltpu.make_async_copy(
        w_hbm.at[pl.ds(pl.multiple_of(r * share, share), share), :], w_v, load_sem.at[2]
    )
    load_a.start()
    load_f.start()
    load_w.start()

    nodes = degree_ref.shape[1]

    def scale_column(first, count):
        start = pl.multiple_of(first // 128 * 128, 128)
        span = up(count + 127, 128)
        window = jnp.broadcast_to(d_v[:, pl.ds(start, span)], (up(count, 8), span))
        lane = lax.broadcasted_iota(jnp.int32, window.shape, 1)
        row = lax.broadcasted_iota(jnp.int32, window.shape, 0)
        picked = jnp.where(lane - row == first - start, window, 0.0)
        return jnp.sum(picked, axis=1, keepdims=True)[:count]

    barrier = pltpu.get_barrier_semaphore()
    peers = [(r, p) for p in others] + [(mate, p) for p in outer + inner] + [(mate, c)]
    peers += [(yy * CORES + k, c) for yy in y_at[:-1]]
    for row, col in peers:
        pl.semaphore_signal(barrier, inc=1, device_id=(row, col), device_id_type=MESH)
    d_v[:, 0:nodes] = lax.rsqrt(degree_ref[...].astype(F32))
    row_scale = scale_column(r * rows + c * block, block)
    for q in range(R):
        piece = cot_ref[:, q * share:(q + 1) * share].astype(F32) * row_scale
        if padded > block:
            piece = jnp.concatenate([piece, jnp.zeros((padded - block, share), F32)], axis=0)
        x_ref[q] = piece.astype(BF16)
    pl.semaphore_wait(barrier, len(peers))

    live = pl.ds(0, padded)
    for s in range(Y):
        same = x_ref.at[y_at[s] * CORES + k]
        cross = x_ref.at[y_at[s] * CORES + (1 - k)]
        for p in outer + inner:
            remote(same, s_v.at[s, 0, c, live], own_sem.at[s, 0], got_sem.at[s, c], r, p).start()
            remote(cross, s_v.at[s, 1, c, live], own_sem.at[s, 1], got_sem.at[s, c], mate, p).start()
        remote(cross, s_v.at[s, 1, c, live], pair_sem.at[s], got_sem.at[s, c], mate, c).start()
        s_v[s, 0, c, 0:padded, :] = x_ref[y_at[s] * CORES + k]
    if slot > padded:
        for s in range(Y):
            s_v[s, :, :, padded:slot, :] = jnp.zeros((CORES, C, slot - padded, share), BF16)

    load_a.wait()
    for j in range(C):
        start = min(j * block, rows - slot)
        tile = a_v[:, start:start + slot]
        if j * block > start:
            tile = pltpu.roll(tile, slot - (j * block - start), 1)
        at[0, :, j * slot:(j + 1) * slot] = tile.astype(F32).astype(BF16)
    swap = remote(at.at[0], at.at[1], swap_sem.at[0], swap_sem.at[1], mate, c)
    swap.start()

    group = min(C, 8)

    def forward(s):
        for d, p in enumerate(outer):
            await_bytes(s_v.at[s, :, p, live], got_sem.at[s, p])
            for q in inner:
                remote(
                    s_v.at[s, :, p, live], s_v.at[s, :, p, live],
                    fwd_sem.at[s, d], got_sem.at[s, p], r, q,
                ).start()

    def gathered(s):
        await_bytes(s_v.at[s, 1, c, live], got_sem.at[s, c])
        for e in range(1, I):
            for d in range(O):
                p = lax.rem(o + d, O) * I + lax.rem(i + e, I)
                await_bytes(s_v.at[s, :, p, live], got_sem.at[s, p])

    def product(s):
        def term(t, g):
            left = at[t, :, pl.ds(pl.multiple_of(g * group * slot, group * slot), group * slot)]
            right = s_v[s, t, pl.ds(g * group, group)].reshape(group * slot, share)
            return jnp.dot(left, right, preferred_element_type=F32)

        if C == group:
            mine[...] = term(0, 0) + term(1, 0)
        else:
            mine[...] = jnp.zeros_like(mine)

            @pl.loop(0, C // group)
            def _(g):
                mine[...] += term(0, g) + term(1, g)

    for s in range(Y):
        forward(s)
        if s == 0:
            load_f.wait()
            ft[...] = f_v[...].astype(F32).T.astype(BF16)
            col_scale = scale_column(c * n, n)
        gathered(s)
        if s == 0:
            swap.wait()
        product(s)
        if s < Y - 1:
            part[s] = mine[...]
            remote(
                part.at[s], theirs.at[s], part_send.at[s], part_recv.at[s], y_at[s] * CORES + k, c
            ).start()

    total = mine[...]
    for s in range(Y - 1):
        await_bytes(theirs.at[s], part_recv.at[s])
        total = total + theirs[s]
    z_mine = (total * col_scale).astype(BF16)
    z_all[r] = z_mine
    z_here = z_all.at[r]
    for s in range(Y - 1):
        remote(z_here, z_here, z_send.at[s], z_recv.at[r], y_at[s] * CORES + k, c).start()
    remote(z_here, z_here, z_send.at[Y - 1], z_recv.at[r], mate, c).start()

    term = jnp.dot(ft[...], z_mine, preferred_element_type=F32)
    wt[...] = term.reshape(wt.shape)
    for p in others:
        remote(wt.at[p], wrec.at[c], wt_send.at[0], wt_recv.at[c], r, p).start()

    for s in range(Y - 1):
        q = y_at[s] * CORES + k
        await_bytes(z_all.at[q], z_recv.at[q])
        remote(z_all.at[q], z_all.at[q], z_fwd.at[s], z_recv.at[q], mate, c).start()
    load_w.wait()
    for s in range(Y):
        q = y_at[s] * CORES + (1 - k)
        await_bytes(z_all.at[q], z_recv.at[q])
    out = jnp.zeros((n, share), F32)
    for q in range(R):
        out = out + lax.dot_general(
            z_all[q], w_v[:, q * share:(q + 1) * share],
            (((1,), (1,)), ((), ())), preferred_element_type=F32,
        )
    gi_ref[...] = out.astype(BF16)

    gw = wt[c]
    for p in others:
        await_bytes(wrec.at[p], wt_recv.at[p])
        gw = gw + wrec[p]
    gw_ref[...] = gw

    for s in range(Y):
        for t in range(CORES):
            await_bytes(s_v.at[s, t, pl.ds(0, O - 1 + I - 1), live], own_sem.at[s, t])
        await_bytes(s_v.at[s, 1, 0, live], pair_sem.at[s])
        if I > 1:
            for d in range(O - 1):
                await_bytes(s_v.at[s, :, pl.ds(0, I - 1), live], fwd_sem.at[s, d])
    for s in range(Y - 1):
        await_bytes(part.at[s], part_send.at[s])
        await_bytes(z_here, z_fwd.at[s])
    for s in range(Y):
        await_bytes(z_here, z_send.at[s])
    await_bytes(wt.at[pl.ds(0, C - 1)], wt_send.at[0])


def per_device(R, C, adjacency, degree, cotangent, features, weight):
    rows, n = adjacency.shape
    block, width = cotangent.shape
    nodes, share = degree.shape[0], width // R
    padded, slot = up(block, 16), up(block, 128)
    I = inner_of(C)
    O, Y = C // I, R // CORES
    vmem = pl.BlockSpec(memory_space=pltpu.VMEM)
    hbm = pl.BlockSpec(memory_space=pltpu.HBM)
    dma = pltpu.SemaphoreType.DMA
    return pl.pallas_call(
        functools.partial(kernel, R, C, block),
        out_shape=(
            jax.ShapeDtypeStruct((n, width // R), BF16),
            jax.ShapeDtypeStruct((width // C, share), F32),
        ),
        in_specs=[vmem, vmem, hbm, hbm, hbm],
        out_specs=(vmem, vmem),
        scratch_shapes=[
            pltpu.VMEM((1, up(nodes, 128) + up(n + 127, 128)), F32),
            pltpu.VMEM((R, padded, share), BF16),
            pltpu.VMEM((n, rows), jnp.int32),
            pltpu.VMEM((n, width), BF16),
            pltpu.VMEM((share, width), BF16),
            pltpu.VMEM((CORES, n, C * slot), BF16),
            pltpu.VMEM((width, n), BF16),
            pltpu.VMEM((Y, CORES, C, slot, share), BF16),
            pltpu.VMEM((n, share), F32),
            pltpu.VMEM((max(Y - 1, 1), n, share), F32),
            pltpu.VMEM((max(Y - 1, 1), n, share), F32),
            pltpu.VMEM((R, n, share), BF16),
            pltpu.VMEM((C, width // C, share), F32),
            pltpu.VMEM((C, width // C, share), F32),
            dma((3,)),
            dma((2,)),
            dma((Y, CORES)),
            dma((Y,)),
            dma((Y, C)),
            dma((Y, max(O - 1, 1))),
            dma((max(Y - 1, 1),)),
            dma((max(Y - 1, 1),)),
            dma((Y,)),
            dma((R,)),
            dma((max(Y - 1, 1),)),
            dma((1,)),
            dma((C,)),
        ],
        compiler_params=pltpu.CompilerParams(
            collective_id=0, has_side_effects=True, vmem_limit_bytes=min(60 << 20, (12 << 20) + 24 * rows * n)
        ),
    )(cotangent, degree.reshape(1, nodes), adjacency.T, features, weight)


def solution(mesh):
    placed = (P("row", "col"), P(), P(("row", "col"), None), P("col", None), P())
    return jax.shard_map(
        functools.partial(per_device, mesh.shape["row"], mesh.shape["col"]),
        mesh=mesh,
        in_specs=placed,
        out_specs=(P("col", "row"), P("col", "row")),
        check_vma=False,
    )
```

```python
import functools

import jax
import jax.numpy as jnp
from jax import lax
from jax.experimental import pallas as pl
from jax.experimental.pallas import tpu as pltpu
from jax.sharding import PartitionSpec as P

MESH = pl.DeviceIdType.MESH
F32, BF16 = jnp.float32, jnp.bfloat16
CORES = 2


def up(size, unit):
    return -(-size // unit) * unit


def inner_of(count):
    return max(d for d in range(1, count + 1) if count % d == 0 and d * d <= count)


def kernel(
    R, C, block,
    cot_hbm, degree_ref, a_hbm, f_hbm, w_hbm, gi_ref, gw_ref,
    d_v, cot_ref, x_ref, a_v, f_v, w_v, at, ft, s_v, mine, part, theirs, z_all, wt, wrec,
    load_sem, swap_sem, own_sem, pair_sem, got_sem, fwd_sem,
    part_send, part_recv, z_send, z_recv, z_fwd, wt_send, wt_recv,
):
    I = inner_of(C)
    O = C // I
    Y = R // CORES
    n, rows = a_v.shape
    padded, share = x_ref.shape[1:]
    slot = s_v.shape[3]
    r = lax.axis_index("row")
    c = lax.axis_index("col")
    y, k = r // CORES, r % CORES
    o, i = c // I, c % I
    mate = y * CORES + (1 - k)
    outer = [lax.rem(o + d, O) * I + i for d in range(1, O)]
    inner = [o * I + lax.rem(i + d, I) for d in range(1, I)]
    others = [lax.rem(c + d, C) for d in range(1, C)]
    y_at = [lax.rem(y + 1 + s, Y) for s in range(Y)]

    def remote(src, dst, send, recv, row, col):
        return pltpu.make_async_remote_copy(
            src_ref=src, dst_ref=dst, send_sem=send, recv_sem=recv,
            device_id=(row, col), device_id_type=MESH,
        )

    def await_bytes(ref, sem):
        pltpu.make_async_copy(ref, ref, sem).wait()

    load_a = pltpu.make_async_copy(a_hbm, a_v, load_sem.at[0])
    load_f = pltpu.make_async_copy(f_hbm, f_v, load_sem.at[1])
    load_w = pltpu.make_async_copy(
        w_hbm.at[pl.ds(pl.multiple_of(r * share, share), share), :], w_v, load_sem.at[2]
    )
    load_c = pltpu.make_async_copy(cot_hbm, cot_ref, load_sem.at[3])
    load_c.start()
    load_a.start()
    load_f.start()
    load_w.start()

    nodes = degree_ref.shape[1]

    def scale_column(first, count):
        start = pl.multiple_of(first // 128 * 128, 128)
        span = up(count + 127, 128)
        window = jnp.broadcast_to(d_v[:, pl.ds(start, span)], (up(count, 8), span))
        lane = lax.broadcasted_iota(jnp.int32, window.shape, 1)
        row = lax.broadcasted_iota(jnp.int32, window.shape, 0)
        picked = jnp.where(lane - row == first - start, window, 0.0)
        return jnp.sum(picked, axis=1, keepdims=True)[:count]

    barrier = pltpu.get_barrier_semaphore()
    peers = [(r, p) for p in others] + [(mate, p) for p in outer + inner] + [(mate, c)]
    peers += [(yy * CORES + k, c) for yy in y_at[:-1]]
    for row, col in peers:
        pl.semaphore_signal(barrier, inc=1, device_id=(row, col), device_id_type=MESH)
    d_v[:, 0:nodes] = lax.rsqrt(degree_ref[...].astype(F32))
    load_c.wait()
    row_scale = scale_column(r * rows + c * block, block)
    for q in range(R):
        piece = cot_ref[:, q * share:(q + 1) * share].astype(F32) * row_scale
        if padded > block:
            piece = jnp.concatenate([piece, jnp.zeros((padded - block, share), F32)], axis=0)
        x_ref[q] = piece.astype(BF16)
    pl.semaphore_wait(barrier, len(peers))

    live = pl.ds(0, padded)
    for s in range(Y):
        same = x_ref.at[y_at[s] * CORES + k]
        cross = x_ref.at[y_at[s] * CORES + (1 - k)]
        for p in outer + inner:
            remote(same, s_v.at[s, 0, c, live], own_sem.at[s, 0], got_sem.at[s, c], r, p).start()
            remote(cross, s_v.at[s, 1, c, live], own_sem.at[s, 1], got_sem.at[s, c], mate, p).start()
        remote(cross, s_v.at[s, 1, c, live], pair_sem.at[s], got_sem.at[s, c], mate, c).start()
        s_v[s, 0, c, 0:padded, :] = x_ref[y_at[s] * CORES + k]
    if slot > padded:
        for s in range(Y):
            s_v[s, :, :, padded:slot, :] = jnp.zeros((CORES, C, slot - padded, share), BF16)

    load_a.wait()
    for j in range(C):
        start = min(j * block, rows - slot)
        tile = a_v[:, start:start + slot]
        if j * block > start:
            tile = pltpu.roll(tile, slot - (j * block - start), 1)
        at[0, :, j * slot:(j + 1) * slot] = tile.astype(F32).astype(BF16)
    swap = remote(at.at[0], at.at[1], swap_sem.at[0], swap_sem.at[1], mate, c)
    swap.start()

    group = min(C, 8)

    def forward(s):
        for d, p in enumerate(outer):
            await_bytes(s_v.at[s, :, p, live], got_sem.at[s, p])
            for q in inner:
                remote(
                    s_v.at[s, :, p, live], s_v.at[s, :, p, live],
                    fwd_sem.at[s, d], got_sem.at[s, p], r, q,
                ).start()

    def gathered(s):
        await_bytes(s_v.at[s, 1, c, live], got_sem.at[s, c])
        for e in range(1, I):
            for d in range(O):
                p = lax.rem(o + d, O) * I + lax.rem(i + e, I)
                await_bytes(s_v.at[s, :, p, live], got_sem.at[s, p])

    def product(s):
        def term(t, g):
            left = at[t, :, pl.ds(pl.multiple_of(g * group * slot, group * slot), group * slot)]
            right = s_v[s, t, pl.ds(g * group, group)].reshape(group * slot, share)
            return jnp.dot(left, right, preferred_element_type=F32)

        if C == group:
            mine[...] = term(0, 0) + term(1, 0)
        else:
            mine[...] = jnp.zeros_like(mine)

            @pl.loop(0, C // group)
            def _(g):
                mine[...] += term(0, g) + term(1, g)

    for s in range(Y):
        forward(s)
        if s == 0:
            load_f.wait()
            ft[...] = f_v[...].astype(F32).T.astype(BF16)
            col_scale = scale_column(c * n, n)
        gathered(s)
        if s == 0:
            swap.wait()
        product(s)
        if s < Y - 1:
            part[s] = mine[...]
            remote(
                part.at[s], theirs.at[s], part_send.at[s], part_recv.at[s], y_at[s] * CORES + k, c
            ).start()

    total = mine[...]
    for s in range(Y - 1):
        await_bytes(theirs.at[s], part_recv.at[s])
        total = total + theirs[s]
    z_mine = (total * col_scale).astype(BF16)
    z_all[r] = z_mine
    z_here = z_all.at[r]
    for s in range(Y - 1):
        remote(z_here, z_here, z_send.at[s], z_recv.at[r], y_at[s] * CORES + k, c).start()
    remote(z_here, z_here, z_send.at[Y - 1], z_recv.at[r], mate, c).start()

    term = jnp.dot(ft[...], z_mine, preferred_element_type=F32)
    wt[...] = term.reshape(wt.shape)
    for p in others:
        remote(wt.at[p], wrec.at[c], wt_send.at[0], wt_recv.at[c], r, p).start()

    for s in range(Y - 1):
        q = y_at[s] * CORES + k
        await_bytes(z_all.at[q], z_recv.at[q])
        remote(z_all.at[q], z_all.at[q], z_fwd.at[s], z_recv.at[q], mate, c).start()
    load_w.wait()
    for s in range(Y):
        q = y_at[s] * CORES + (1 - k)
        await_bytes(z_all.at[q], z_recv.at[q])
    out = jnp.zeros((n, share), F32)
    for q in range(R):
        out = out + lax.dot_general(
            z_all[q], w_v[:, q * share:(q + 1) * share],
            (((1,), (1,)), ((), ())), preferred_element_type=F32,
        )
    gi_ref[...] = out.astype(BF16)

    gw = wt[c]
    for p in others:
        await_bytes(wrec.at[p], wt_recv.at[p])
        gw = gw + wrec[p]
    gw_ref[...] = gw

    for s in range(Y):
        for t in range(CORES):
            await_bytes(s_v.at[s, t, pl.ds(0, O - 1 + I - 1), live], own_sem.at[s, t])
        await_bytes(s_v.at[s, 1, 0, live], pair_sem.at[s])
        if I > 1:
            for d in range(O - 1):
                await_bytes(s_v.at[s, :, pl.ds(0, I - 1), live], fwd_sem.at[s, d])
    for s in range(Y - 1):
        await_bytes(part.at[s], part_send.at[s])
        await_bytes(z_here, z_fwd.at[s])
    for s in range(Y):
        await_bytes(z_here, z_send.at[s])
    await_bytes(wt.at[pl.ds(0, C - 1)], wt_send.at[0])


def per_device(R, C, adjacency, degree, cotangent, features, weight):
    rows, n = adjacency.shape
    block, width = cotangent.shape
    nodes, share = degree.shape[0], width // R
    padded, slot = up(block, 16), up(block, 128)
    I = inner_of(C)
    O, Y = C // I, R // CORES
    results = up(n, 16) * up(share, 128) * 2 + up(width // C, 8) * up(share, 128) * 4
    vmem = pl.BlockSpec(memory_space=pltpu.VMEM)
    hbm = pl.BlockSpec(memory_space=pltpu.HBM)
    dma = pltpu.SemaphoreType.DMA
    return pl.pallas_call(
        functools.partial(kernel, R, C, block),
        out_shape=(
            jax.ShapeDtypeStruct((n, width // R), BF16),
            jax.ShapeDtypeStruct((width // C, share), F32),
        ),
        in_specs=[hbm, vmem, hbm, hbm, hbm],
        out_specs=(vmem, vmem),
        scratch_shapes=[
            pltpu.VMEM((1, up(nodes, 128) + up(n + 127, 128)), F32),
            pltpu.VMEM((block, width), BF16),
            pltpu.VMEM((R, padded, share), BF16),
            pltpu.VMEM((n, rows), jnp.int32),
            pltpu.VMEM((n, width), BF16),
            pltpu.VMEM((share, width), BF16),
            pltpu.VMEM((CORES, n, C * slot), BF16),
            pltpu.VMEM((width, n), BF16),
            pltpu.VMEM((Y, CORES, C, slot, share), BF16),
            pltpu.VMEM((n, share), F32),
            pltpu.VMEM((max(Y - 1, 1), n, share), F32),
            pltpu.VMEM((max(Y - 1, 1), n, share), F32),
            pltpu.VMEM((R, n, share), BF16),
            pltpu.VMEM((C, width // C, share), F32),
            pltpu.VMEM((C, width // C, share), F32),
            dma((4,)),
            dma((2,)),
            dma((Y, CORES)),
            dma((Y,)),
            dma((Y, C)),
            dma((Y, max(O - 1, 1))),
            dma((max(Y - 1, 1),)),
            dma((max(Y - 1, 1),)),
            dma((Y,)),
            dma((R,)),
            dma((max(Y - 1, 1),)),
            dma((1,)),
            dma((C,)),
        ],
        compiler_params=pltpu.CompilerParams(
            collective_id=0, has_side_effects=True, vmem_limit_bytes=56300000
        ),
    )(cotangent, degree.reshape(1, nodes), adjacency.T, features, weight)


def solution(mesh):
    placed = (P("row", "col"), P(), P(("row", "col"), None), P("col", None), P())
    return jax.shard_map(
        functools.partial(per_device, mesh.shape["row"], mesh.shape["col"]),
        mesh=mesh,
        in_specs=placed,
        out_specs=(P("col", "row"), P("col", "row")),
        check_vma=False,
    )
```

```python
import functools

import jax
import jax.numpy as jnp
from jax import lax
from jax.experimental import pallas as pl
from jax.experimental.pallas import tpu as pltpu
from jax.sharding import PartitionSpec as P

MESH = pl.DeviceIdType.MESH
F32, BF16 = jnp.float32, jnp.bfloat16
CORES = 2


def up(size, unit):
    return -(-size // unit) * unit


def inner_of(count):
    return max(d for d in range(1, count + 1) if count % d == 0 and d * d <= count)


def kernel(
    R, C, block,
    cot_hbm, degree_ref, a_hbm, f_hbm, w_hbm, gi_ref, gw_ref,
    d_v, cot_ref, x_ref, a_v, f_v, w_v, at, ft, s_v, mine, part, theirs, z_all, wt, wrec,
    load_sem, swap_sem, own_sem, pair_sem, got_sem, fwd_sem,
    part_send, part_recv, z_send, z_recv, z_fwd, wt_send, wt_recv,
):
    I = inner_of(C)
    O = C // I
    Y = R // CORES
    n, rows = a_v.shape
    padded, share = x_ref.shape[1:]
    slot = s_v.shape[3]
    r = lax.axis_index("row")
    c = lax.axis_index("col")
    y, k = r // CORES, r % CORES
    o, i = c // I, c % I
    mate = y * CORES + (1 - k)
    if O == 4:
        near = [1 + o % 2, (2 + 3 * o) % 5, 3 - 3 * (o // 2)]
    else:
        near = [(o + d) % O for d in range(1, O)]
    outer = [p * I + i for p in near]
    inner = [o * I + lax.rem(i + d, I) for d in range(1, I)]
    others = [lax.rem(c + d, C) for d in range(1, C)]
    y_at = [lax.rem(y + 1 + s, Y) for s in range(Y)]

    def remote(src, dst, send, recv, row, col):
        return pltpu.make_async_remote_copy(
            src_ref=src, dst_ref=dst, send_sem=send, recv_sem=recv,
            device_id=(row, col), device_id_type=MESH,
        )

    def await_bytes(ref, sem):
        pltpu.make_async_copy(ref, ref, sem).wait()

    load_a = pltpu.make_async_copy(a_hbm, a_v, load_sem.at[0])
    load_f = pltpu.make_async_copy(f_hbm, f_v, load_sem.at[1])
    load_w = pltpu.make_async_copy(
        w_hbm.at[pl.ds(pl.multiple_of(r * share, share), share), :], w_v, load_sem.at[2]
    )
    load_c = pltpu.make_async_copy(cot_hbm, cot_ref, load_sem.at[3])
    load_c.start()
    load_a.start()
    load_f.start()
    load_w.start()

    nodes = degree_ref.shape[1]

    def scale_column(first, count):
        start = pl.multiple_of(first // 128 * 128, 128)
        span = up(count + 127, 128)
        window = jnp.broadcast_to(d_v[:, pl.ds(start, span)], (up(count, 8), span))
        lane = lax.broadcasted_iota(jnp.int32, window.shape, 1)
        row = lax.broadcasted_iota(jnp.int32, window.shape, 0)
        picked = jnp.where(lane - row == first - start, window, 0.0)
        return jnp.sum(picked, axis=1, keepdims=True)[:count]

    barrier = pltpu.get_barrier_semaphore()
    peers = [(r, p) for p in others] + [(mate, p) for p in outer + inner] + [(mate, c)]
    peers += [(yy * CORES + k, c) for yy in y_at[:-1]]
    for row, col in peers:
        pl.semaphore_signal(barrier, inc=1, device_id=(row, col), device_id_type=MESH)
    d_v[:, 0:nodes] = lax.rsqrt(degree_ref[...].astype(F32))
    load_c.wait()
    row_scale = scale_column(r * rows + c * block, block)
    for q in range(R):
        piece = cot_ref[:, q * share:(q + 1) * share].astype(F32) * row_scale
        if padded > block:
            piece = jnp.concatenate([piece, jnp.zeros((padded - block, share), F32)], axis=0)
        x_ref[q] = piece.astype(BF16)
    pl.semaphore_wait(barrier, len(peers))

    live = pl.ds(0, padded)
    for s in range(Y):
        same = x_ref.at[y_at[s] * CORES + k]
        cross = x_ref.at[y_at[s] * CORES + (1 - k)]
        for p in outer + inner:
            remote(same, s_v.at[s, 0, c, live], own_sem.at[s, 0], got_sem.at[s, c], r, p).start()
            remote(cross, s_v.at[s, 1, c, live], own_sem.at[s, 1], got_sem.at[s, c], mate, p).start()
        remote(cross, s_v.at[s, 1, c, live], pair_sem.at[s], got_sem.at[s, c], mate, c).start()
        s_v[s, 0, c, 0:padded, :] = x_ref[y_at[s] * CORES + k]
    if slot > padded:
        for s in range(Y):
            s_v[s, :, :, padded:slot, :] = jnp.zeros((CORES, C, slot - padded, share), BF16)

    load_a.wait()
    for j in range(C):
        start = min(j * block, rows - slot)
        tile = a_v[:, start:start + slot]
        if j * block > start:
            tile = pltpu.roll(tile, slot - (j * block - start), 1)
        at[0, :, j * slot:(j + 1) * slot] = tile.astype(F32).astype(BF16)
    swap = remote(at.at[0], at.at[1], swap_sem.at[0], swap_sem.at[1], mate, c)
    swap.start()

    group = min(C, 8)

    def forward(s):
        for d, p in enumerate(outer):
            await_bytes(s_v.at[s, :, p, live], got_sem.at[s, p])
            for q in inner:
                remote(
                    s_v.at[s, :, p, live], s_v.at[s, :, p, live],
                    fwd_sem.at[s, d], got_sem.at[s, p], r, q,
                ).start()

    def gathered(s):
        await_bytes(s_v.at[s, 1, c, live], got_sem.at[s, c])
        for e in range(1, I):
            for d in range(O):
                p = lax.rem(o + d, O) * I + lax.rem(i + e, I)
                await_bytes(s_v.at[s, :, p, live], got_sem.at[s, p])

    def product(s):
        def term(t, g):
            left = at[t, :, pl.ds(pl.multiple_of(g * group * slot, group * slot), group * slot)]
            right = s_v[s, t, pl.ds(g * group, group)].reshape(group * slot, share)
            return jnp.dot(left, right, preferred_element_type=F32)

        if C == group:
            mine[...] = term(0, 0) + term(1, 0)
        else:
            mine[...] = jnp.zeros_like(mine)

            @pl.loop(0, C // group)
            def _(g):
                mine[...] += term(0, g) + term(1, g)

    forward(0)
    load_f.wait()
    ft[...] = f_v[...].astype(F32).T.astype(BF16)
    col_scale = scale_column(c * n, n)
    for s in range(1, Y):
        forward(s)
    for s in range(Y):
        gathered(s)
        if s == 0:
            swap.wait()
        product(s)
        if s < Y - 1:
            part[s] = mine[...]
            remote(
                part.at[s], theirs.at[s], part_send.at[s], part_recv.at[s], y_at[s] * CORES + k, c
            ).start()

    total = mine[...]
    for s in range(Y - 1):
        await_bytes(theirs.at[s], part_recv.at[s])
        total = total + theirs[s]
    z_mine = (total * col_scale).astype(BF16)
    z_all[r] = z_mine
    z_here = z_all.at[r]
    for s in range(Y - 1):
        remote(z_here, z_here, z_send.at[s], z_recv.at[r], y_at[s] * CORES + k, c).start()
    remote(z_here, z_here, z_send.at[Y - 1], z_recv.at[r], mate, c).start()

    term = jnp.dot(ft[...], z_mine, preferred_element_type=F32)
    wt[...] = term.reshape(wt.shape)
    for p in others:
        remote(wt.at[p], wrec.at[c], wt_send.at[0], wt_recv.at[c], r, p).start()

    for s in range(Y - 1):
        q = y_at[s] * CORES + k
        await_bytes(z_all.at[q], z_recv.at[q])
        remote(z_all.at[q], z_all.at[q], z_fwd.at[s], z_recv.at[q], mate, c).start()
    load_w.wait()
    for s in range(Y):
        q = y_at[s] * CORES + (1 - k)
        await_bytes(z_all.at[q], z_recv.at[q])
    out = jnp.zeros((n, share), F32)
    for q in range(R):
        out = out + lax.dot_general(
            z_all[q], w_v[:, q * share:(q + 1) * share],
            (((1,), (1,)), ((), ())), preferred_element_type=F32,
        )
    gi_ref[...] = out.astype(BF16)

    gw = wt[c]
    for p in others:
        await_bytes(wrec.at[p], wt_recv.at[p])
        gw = gw + wrec[p]
    gw_ref[...] = gw

    for s in range(Y):
        for t in range(CORES):
            await_bytes(s_v.at[s, t, pl.ds(0, O - 1 + I - 1), live], own_sem.at[s, t])
        await_bytes(s_v.at[s, 1, 0, live], pair_sem.at[s])
        if I > 1:
            for d in range(O - 1):
                await_bytes(s_v.at[s, :, pl.ds(0, I - 1), live], fwd_sem.at[s, d])
    for s in range(Y - 1):
        await_bytes(part.at[s], part_send.at[s])
        await_bytes(z_here, z_fwd.at[s])
    for s in range(Y):
        await_bytes(z_here, z_send.at[s])
    await_bytes(wt.at[pl.ds(0, C - 1)], wt_send.at[0])


def per_device(R, C, adjacency, degree, cotangent, features, weight):
    rows, n = adjacency.shape
    block, width = cotangent.shape
    nodes, share = degree.shape[0], width // R
    padded, slot = up(block, 16), up(block, 128)
    I = inner_of(C)
    O, Y = C // I, R // CORES
    results = up(n, 16) * up(share, 128) * 2 + up(width // C, 8) * up(share, 128) * 4
    vmem = pl.BlockSpec(memory_space=pltpu.VMEM)
    hbm = pl.BlockSpec(memory_space=pltpu.HBM)
    dma = pltpu.SemaphoreType.DMA
    return pl.pallas_call(
        functools.partial(kernel, R, C, block),
        out_shape=(
            jax.ShapeDtypeStruct((n, width // R), BF16),
            jax.ShapeDtypeStruct((width // C, share), F32),
        ),
        in_specs=[hbm, vmem, hbm, hbm, hbm],
        out_specs=(vmem, vmem),
        scratch_shapes=[
            pltpu.VMEM((1, up(nodes, 128) + up(n + 127, 128)), F32),
            pltpu.VMEM((block, width), BF16),
            pltpu.VMEM((R, padded, share), BF16),
            pltpu.VMEM((n, rows), jnp.int32),
            pltpu.VMEM((n, width), BF16),
            pltpu.VMEM((share, width), BF16),
            pltpu.VMEM((CORES, n, C * slot), BF16),
            pltpu.VMEM((width, n), BF16),
            pltpu.VMEM((Y, CORES, C, slot, share), BF16),
            pltpu.VMEM((n, share), F32),
            pltpu.VMEM((max(Y - 1, 1), n, share), F32),
            pltpu.VMEM((max(Y - 1, 1), n, share), F32),
            pltpu.VMEM((R, n, share), BF16),
            pltpu.VMEM((C, width // C, share), F32),
            pltpu.VMEM((C, width // C, share), F32),
            dma((4,)),
            dma((2,)),
            dma((Y, CORES)),
            dma((Y,)),
            dma((Y, C)),
            dma((Y, max(O - 1, 1))),
            dma((max(Y - 1, 1),)),
            dma((max(Y - 1, 1),)),
            dma((Y,)),
            dma((R,)),
            dma((max(Y - 1, 1),)),
            dma((1,)),
            dma((C,)),
        ],
        compiler_params=pltpu.CompilerParams(
            collective_id=0, has_side_effects=True, vmem_limit_bytes=56300000
        ),
    )(cotangent, degree.reshape(1, nodes), adjacency.T, features, weight)


def solution(mesh):
    placed = (P("row", "col"), P(), P(("row", "col"), None), P("col", None), P())
    return jax.shard_map(
        functools.partial(per_device, mesh.shape["row"], mesh.shape["col"]),
        mesh=mesh,
        in_specs=placed,
        out_specs=(P("col", "row"), P("col", "row")),
        check_vma=False,
    )
```

```python
import functools

import jax
import jax.numpy as jnp
from jax import lax
from jax.experimental import pallas as pl
from jax.experimental.pallas import tpu as pltpu
from jax.sharding import PartitionSpec as P

MESH = pl.DeviceIdType.MESH
F32, BF16 = jnp.float32, jnp.bfloat16
CORES = 2


def up(size, unit):
    return -(-size // unit) * unit


def inner_of(count):
    return max(d for d in range(1, count + 1) if count % d == 0 and d * d <= count)


def kernel(
    R, C, block,
    cot_hbm, degree_ref, a_hbm, f_hbm, w_hbm, gi_ref, gw_ref,
    d_v, cot_ref, x_ref, a_v, f_v, w_v, at, ft, s_v, mine, part, theirs, z_all, wt, wrec,
    load_sem, swap_sem, own_sem, pair_sem, got_sem, fwd_sem,
    part_send, part_recv, z_send, z_recv, z_fwd, wt_send, wt_recv,
):
    I = inner_of(C)
    O = C // I
    Y = R // CORES
    n, rows = a_v.shape
    padded, share = x_ref.shape[1:]
    slot = s_v.shape[3]
    r = lax.axis_index("row")
    c = lax.axis_index("col")
    y, k = r // CORES, r % CORES
    o, i = c // I, c % I
    mate = y * CORES + (1 - k)
    if O == 4:
        near = [1 + o % 2, (2 + 3 * o) % 5, 3 - 3 * (o // 2)]
    else:
        near = [(o + d) % O for d in range(1, O)]
    outer = [p * I + i for p in near]
    inner = [o * I + lax.rem(i + d, I) for d in range(1, I)]
    others = [lax.rem(c + d, C) for d in range(1, C)]
    y_at = [lax.rem(y + 1 + s, Y) for s in range(Y)]

    def remote(src, dst, send, recv, row, col):
        return pltpu.make_async_remote_copy(
            src_ref=src, dst_ref=dst, send_sem=send, recv_sem=recv,
            device_id=(row, col), device_id_type=MESH,
        )

    def await_bytes(ref, sem):
        pltpu.make_async_copy(ref, ref, sem).wait()

    load_a = pltpu.make_async_copy(a_hbm, a_v, load_sem.at[0])
    load_f = pltpu.make_async_copy(f_hbm, f_v, load_sem.at[1])
    load_w = pltpu.make_async_copy(
        w_hbm.at[pl.ds(pl.multiple_of(r * share, share), share), :], w_v, load_sem.at[2]
    )
    load_c = pltpu.make_async_copy(cot_hbm, cot_ref, load_sem.at[3])
    load_c.start()
    load_a.start()
    load_f.start()
    load_w.start()

    nodes = degree_ref.shape[1]

    def scale_column(first, count):
        start = pl.multiple_of(first // 128 * 128, 128)
        span = up(count + 127, 128)
        window = jnp.broadcast_to(d_v[:, pl.ds(start, span)], (up(count, 8), span))
        lane = lax.broadcasted_iota(jnp.int32, window.shape, 1)
        row = lax.broadcasted_iota(jnp.int32, window.shape, 0)
        picked = jnp.where(lane - row == first - start, window, 0.0)
        return jnp.sum(picked, axis=1, keepdims=True)[:count]

    barrier = pltpu.get_barrier_semaphore()
    peers = [(r, p) for p in others] + [(mate, p) for p in outer + inner] + [(mate, c)]
    peers += [(yy * CORES + k, c) for yy in y_at[:-1]]
    for row, col in peers:
        pl.semaphore_signal(barrier, inc=1, device_id=(row, col), device_id_type=MESH)
    d_v[:, 0:nodes] = lax.rsqrt(degree_ref[...].astype(F32))
    load_c.wait()
    row_scale = scale_column(r * rows + c * block, block)
    for q in range(R):
        piece = cot_ref[:, q * share:(q + 1) * share].astype(F32) * row_scale
        if padded > block:
            piece = jnp.concatenate([piece, jnp.zeros((padded - block, share), F32)], axis=0)
        x_ref[q] = piece.astype(BF16)
    pl.semaphore_wait(barrier, len(peers))

    live = pl.ds(0, padded)
    for s in range(Y):
        same = x_ref.at[y_at[s] * CORES + k]
        cross = x_ref.at[y_at[s] * CORES + (1 - k)]
        for p in outer + inner:
            remote(same, s_v.at[s, 0, c, live], own_sem.at[s, 0], got_sem.at[s, c], r, p).start()
            remote(cross, s_v.at[s, 1, c, live], own_sem.at[s, 1], got_sem.at[s, c], mate, p).start()
        remote(cross, s_v.at[s, 1, c, live], pair_sem.at[s], got_sem.at[s, c], mate, c).start()
        s_v[s, 0, c, 0:padded, :] = x_ref[y_at[s] * CORES + k]
    if slot > padded:
        for s in range(Y):
            s_v[s, :, :, padded:slot, :] = jnp.zeros((CORES, C, slot - padded, share), BF16)

    load_a.wait()
    for j in range(C):
        start = min(j * block, rows - slot)
        tile = a_v[:, start:start + slot]
        if j * block > start:
            tile = pltpu.roll(tile, slot - (j * block - start), 1)
        at[0, :, j * slot:(j + 1) * slot] = tile.astype(F32).astype(BF16)
    swap = remote(at.at[0], at.at[1], swap_sem.at[0], swap_sem.at[1], mate, c)
    swap.start()

    group = min(C, 8)

    def forward(s):
        for d, p in enumerate(outer):
            await_bytes(s_v.at[s, :, p, live], got_sem.at[s, p])
            for q in inner:
                remote(
                    s_v.at[s, :, p, live], s_v.at[s, :, p, live],
                    fwd_sem.at[s, d], got_sem.at[s, p], r, q,
                ).start()

    def gathered(s):
        await_bytes(s_v.at[s, 1, c, live], got_sem.at[s, c])
        for e in range(1, I):
            for d in range(O):
                p = lax.rem(o + d, O) * I + lax.rem(i + e, I)
                await_bytes(s_v.at[s, :, p, live], got_sem.at[s, p])

    def product(s):
        def term(t, g):
            left = at[t, :, pl.ds(pl.multiple_of(g * group * slot, group * slot), group * slot)]
            right = s_v[s, t, pl.ds(g * group, group)].reshape(group * slot, share)
            return jnp.dot(left, right, preferred_element_type=F32)

        if C == group:
            mine[...] = term(0, 0) + term(1, 0)
        else:
            mine[...] = jnp.zeros_like(mine)

            @pl.loop(0, C // group)
            def _(g):
                mine[...] += term(0, g) + term(1, g)

    forward(0)
    load_f.wait()
    ft[...] = f_v[...].astype(F32).T.astype(BF16)
    col_scale = scale_column(c * n, n)
    for s in range(1, Y):
        forward(s)
    for s in range(Y):
        gathered(s)
        if s == 0:
            swap.wait()
        product(s)
        if s < Y - 1:
            part[s] = mine[...].astype(BF16)
            remote(
                part.at[s], theirs.at[s], part_send.at[s], part_recv.at[s], y_at[s] * CORES + k, c
            ).start()

    total = mine[...]
    for s in range(Y - 1):
        await_bytes(theirs.at[s], part_recv.at[s])
        total = total + theirs[s].astype(F32)
    z_mine = (total * col_scale).astype(BF16)
    z_all[r] = z_mine
    z_here = z_all.at[r]
    for s in range(Y - 1):
        remote(z_here, z_here, z_send.at[s], z_recv.at[r], y_at[s] * CORES + k, c).start()
    remote(z_here, z_here, z_send.at[Y - 1], z_recv.at[r], mate, c).start()

    term = jnp.dot(ft[...], z_mine, preferred_element_type=F32)
    wt[...] = term.reshape(wt.shape)
    for p in others:
        remote(wt.at[p], wrec.at[c], wt_send.at[0], wt_recv.at[c], r, p).start()

    for s in range(Y - 1):
        q = y_at[s] * CORES + k
        await_bytes(z_all.at[q], z_recv.at[q])
        remote(z_all.at[q], z_all.at[q], z_fwd.at[s], z_recv.at[q], mate, c).start()
    load_w.wait()
    for s in range(Y):
        q = y_at[s] * CORES + (1 - k)
        await_bytes(z_all.at[q], z_recv.at[q])
    out = jnp.zeros((n, share), F32)
    for q in range(R):
        out = out + lax.dot_general(
            z_all[q], w_v[:, q * share:(q + 1) * share],
            (((1,), (1,)), ((), ())), preferred_element_type=F32,
        )
    gi_ref[...] = out.astype(BF16)

    gw = wt[c]
    for p in others:
        await_bytes(wrec.at[p], wt_recv.at[p])
        gw = gw + wrec[p]
    gw_ref[...] = gw

    for s in range(Y):
        for t in range(CORES):
            await_bytes(s_v.at[s, t, pl.ds(0, O - 1 + I - 1), live], own_sem.at[s, t])
        await_bytes(s_v.at[s, 1, 0, live], pair_sem.at[s])
        if I > 1:
            for d in range(O - 1):
                await_bytes(s_v.at[s, :, pl.ds(0, I - 1), live], fwd_sem.at[s, d])
    for s in range(Y - 1):
        await_bytes(part.at[s], part_send.at[s])
        await_bytes(z_here, z_fwd.at[s])
    for s in range(Y):
        await_bytes(z_here, z_send.at[s])
    await_bytes(wt.at[pl.ds(0, C - 1)], wt_send.at[0])


def per_device(R, C, adjacency, degree, cotangent, features, weight):
    rows, n = adjacency.shape
    block, width = cotangent.shape
    nodes, share = degree.shape[0], width // R
    padded, slot = up(block, 16), up(block, 128)
    I = inner_of(C)
    O, Y = C // I, R // CORES
    results = up(n, 16) * up(share, 128) * 2 + up(width // C, 8) * up(share, 128) * 4
    vmem = pl.BlockSpec(memory_space=pltpu.VMEM)
    hbm = pl.BlockSpec(memory_space=pltpu.HBM)
    dma = pltpu.SemaphoreType.DMA
    return pl.pallas_call(
        functools.partial(kernel, R, C, block),
        out_shape=(
            jax.ShapeDtypeStruct((n, width // R), BF16),
            jax.ShapeDtypeStruct((width // C, share), F32),
        ),
        in_specs=[hbm, vmem, hbm, hbm, hbm],
        out_specs=(vmem, vmem),
        scratch_shapes=[
            pltpu.VMEM((1, up(nodes, 128) + up(n + 127, 128)), F32),
            pltpu.VMEM((block, width), BF16),
            pltpu.VMEM((R, padded, share), BF16),
            pltpu.VMEM((n, rows), jnp.int32),
            pltpu.VMEM((n, width), BF16),
            pltpu.VMEM((share, width), BF16),
            pltpu.VMEM((CORES, n, C * slot), BF16),
            pltpu.VMEM((width, n), BF16),
            pltpu.VMEM((Y, CORES, C, slot, share), BF16),
            pltpu.VMEM((n, share), F32),
            pltpu.VMEM((max(Y - 1, 1), n, share), BF16),
            pltpu.VMEM((max(Y - 1, 1), n, share), BF16),
            pltpu.VMEM((R, n, share), BF16),
            pltpu.VMEM((C, width // C, share), F32),
            pltpu.VMEM((C, width // C, share), F32),
            dma((4,)),
            dma((2,)),
            dma((Y, CORES)),
            dma((Y,)),
            dma((Y, C)),
            dma((Y, max(O - 1, 1))),
            dma((max(Y - 1, 1),)),
            dma((max(Y - 1, 1),)),
            dma((Y,)),
            dma((R,)),
            dma((max(Y - 1, 1),)),
            dma((1,)),
            dma((C,)),
        ],
        compiler_params=pltpu.CompilerParams(
            collective_id=0, has_side_effects=True, vmem_limit_bytes=56300000
        ),
    )(cotangent, degree.reshape(1, nodes), adjacency.T, features, weight)


def solution(mesh):
    placed = (P("row", "col"), P(), P(("row", "col"), None), P("col", None), P())
    return jax.shard_map(
        functools.partial(per_device, mesh.shape["row"], mesh.shape["col"]),
        mesh=mesh,
        in_specs=placed,
        out_specs=(P("col", "row"), P("col", "row")),
        check_vma=False,
    )
```
